32 devices in a mesh: band: 16 (over z, y, x), chan: 2 (over core).
Axes of the slice: x: 2, y: 2, z: 4, core: 2. Of those that a mesh axis runs over, the one named last changes fastest.
Arguments:
- grid_latent: bfloat16 [18432, 512], P(('band', 'chan')), may hold values from -6 to 6
- edge_latent: bfloat16 [36864, 512], P(('band', 'chan')), may hold values from -6 to 6
- mesh_latent: bfloat16 [5120, 512], P(('band', 'chan')), may hold values from -6 to 6
- mesh_cotangent: bfloat16 [5120, 512], P(('band', 'chan')), may hold values from -6 to 6
- w_grid: bfloat16 [512, 512], P(None, 'chan'), may hold values from -0.15625 to 0.15625
- w_mesh: bfloat16 [512, 512], P(None, 'chan'), may hold values from -0.15625 to 0.15625
- w_edge: bfloat16 [512, 512], P(None, 'chan'), may hold values from -0.15625 to 0.15625
- bias: float32 [512], P('chan'), may hold values from -3 to 3
- w_out: bfloat16 [512, 512], P('chan'), may hold values from -0.25 to 0.25
- senders: int32 [36864], P('band'), may hold values from 0 to 18431, as said below
- receivers: int32 [36864], P('band'), may hold values from 0 to 5119, as said below
- edge_count: int32 [16], P('band'), may hold values from 1152 to 2304, as said below
Outputs:
- grad_grid: bfloat16 [18432, 512], P(('band', 'chan'))
- grad_edge: bfloat16 [36864, 512], P(('band', 'chan'))
- grad_mesh: bfloat16 [5120, 512], P(('band', 'chan'))
- grad_w_grid: float32 [512, 512], P(None, 'chan')
- grad_w_mesh: float32 [512, 512], P(None, 'chan')
- grad_w_edge: float32 [512, 512], P(None, 'chan')
- grad_bias: float32 [512], P('chan')
- grad_w_out: float32 [512, 512], P('chan')
The draws below stay inside these ranges and needn't reach their ends.
Inputs may be any that keep to these rules, and one draw needn't show every extreme that they name: `senders`: an edge of band j (rows j * 2304 to (j + 1) * 2304 - 1) has its sender among grid rows j * 1152 to (j + 1) * 1152 - 1. `receivers`: an edge of band j has its receiver among mesh rows of owners j - 1, j, j + 1 (owner i holds rows i * 320 to (i + 1) * 320 - 1). `edge_count`: some band uses all 2304 slots.
All inputs are finite; a program needn't handle non-finite values.
Results may differ from the reference program's by a relative error of at most 0.0059.
Values may be sent and summed in bfloat16 or wider, within the bound.
A program may use at most 64 MiB of HBM per device.

```python
import jax
import jax.numpy as jnp
from jax import lax

D = 512
H = 512
E_DEV = 2304
MB = 320
G_DEV = 1152
EDGES = 36864
GRID = 18432
MESH = 5120
N_CHAN = 2


def draw_senders(key, part):
    band_of = jnp.arange(EDGES, dtype=jnp.int32) // E_DEV
    return band_of * G_DEV + jax.random.randint(key, (EDGES,), 0, G_DEV, dtype=jnp.int32)


def draw_receivers(key, part):
    first, second = jax.random.split(jax.random.fold_in(key, 11))
    band_of = jnp.arange(EDGES, dtype=jnp.int32) // E_DEV
    offset = jax.random.randint(first, (EDGES,), -1, 2, dtype=jnp.int32)
    owner = jnp.clip(band_of + offset, 0, EDGES // E_DEV - 1)
    return owner * MB + jax.random.randint(second, (EDGES,), 0, MB, dtype=jnp.int32)


def draw_edge_count(key, part):
    first, second = jax.random.split(jax.random.fold_in(key, 23))
    bands = EDGES // E_DEV
    counts = jax.random.randint(first, (bands,), E_DEV // 2, E_DEV + 1, dtype=jnp.int32)
    fullest = jax.random.randint(second, (), 0, bands, dtype=jnp.int32)
    return jnp.where(jnp.arange(bands, dtype=jnp.int32) == fullest, E_DEV, counts)


def steps_of(key, extent, cuts, smallest, top_value):
    factor_of = 1.0
    for position, parts in cuts:
        steps = jax.random.uniform(jax.random.fold_in(jax.random.fold_in(key, 6), position), (parts,), jnp.float32, smallest / len(cuts), top_value / len(cuts))
        factor_of = factor_of * jnp.repeat(jnp.exp(steps), extent[position] // parts).reshape((-1,) + (1,) * (len(extent) - 1 - position))
    return factor_of


def normal_values(stream_key, shape, scale, reach, cuts=(), kind=jnp.bfloat16):
    drawn = jax.random.normal(stream_key, shape, jnp.float32) * scale
    if len(cuts) > 0:
        drawn = steps_of(stream_key, shape, cuts, -0.22, 0.18) * drawn
    return jnp.clip(drawn, min=-reach, max=reach).astype(kind)


def setup_inputs(seed: int = 0) -> dict:
    arg_keys = jax.random.split(jax.random.key(seed), 13)
    return {
        "grid_latent": normal_values(arg_keys[0], (GRID, D), 1.0, 6.0, ((0, 32),)),
        "edge_latent": normal_values(arg_keys[1], (EDGES, D), 1.0, 6.0, ((0, 32),)),
        "mesh_latent": normal_values(arg_keys[2], (MESH, D), 1.0, 6.0, ((0, 32),)),
        "mesh_cotangent": normal_values(arg_keys[3], (MESH, D), 1.0, 6.0, ((0, 32),)),
        "w_grid": normal_values(arg_keys[4], (D, H), (3 * D) ** -0.5, 0.15625, ((1, 2),)),
        "w_mesh": normal_values(arg_keys[5], (D, H), (3 * D) ** -0.5, 0.15625, ((1, 2),)),
        "w_edge": normal_values(arg_keys[6], (D, H), (3 * D) ** -0.5, 0.15625, ((1, 2),)),
        "bias": normal_values(arg_keys[7], (H,), 0.7, 3.0, ((0, 2),), jnp.float32),
        "w_out": normal_values(arg_keys[8], (H, D), H ** -0.5, 0.25, ((0, 2),)),
        "senders": draw_senders(jax.random.fold_in(arg_keys[12], 71), 0),
        "receivers": draw_receivers(jax.random.fold_in(arg_keys[12], 71), 0),
        "edge_count": draw_edge_count(jax.random.fold_in(arg_keys[12], 71), 0),
    }


def reference(grid_latent, edge_latent, mesh_latent, mesh_cotangent, w_grid, w_mesh, w_edge, bias, w_out, senders, receivers, edge_count):
    rows = jnp.arange(EDGES, dtype=jnp.int32)
    live = (rows % E_DEV) < edge_count[rows // E_DEV]
    gsend = grid_latent[senders]
    mrecv = mesh_latent[receivers]
    pre = (jnp.dot(gsend, w_grid, preferred_element_type=jnp.float32)
           + jnp.dot(mrecv, w_mesh, preferred_element_type=jnp.float32)
           + jnp.dot(edge_latent, w_edge, preferred_element_type=jnp.float32) + bias)
    sig = jax.nn.sigmoid(pre)
    act = (pre * sig).astype(jnp.bfloat16)
    message_cot = jnp.where(live[:, None], mesh_cotangent[receivers], jnp.zeros((), jnp.bfloat16))
    hidden_cot = jnp.dot(message_cot, w_out.T, preferred_element_type=jnp.float32)
    pre_cot = (hidden_cot * sig * (1.0 + pre * (1.0 - sig))).astype(jnp.bfloat16)
    grad_w_grid = jnp.dot(gsend.T, pre_cot, preferred_element_type=jnp.float32)
    grad_w_mesh = jnp.dot(mrecv.T, pre_cot, preferred_element_type=jnp.float32)
    grad_w_edge = jnp.dot(edge_latent.T, pre_cot, preferred_element_type=jnp.float32)
    grad_w_out = jnp.dot(act.T, message_cot, preferred_element_type=jnp.float32)
    grad_bias = jnp.sum(pre_cot.astype(jnp.float32), axis=0)
    group = H // N_CHAN
    edge_total = jnp.zeros((EDGES, D), jnp.float32)
    grid_total = jnp.zeros((GRID, D), jnp.float32)
    for index in range(N_CHAN):
        part_cot = pre_cot[:, index * group:(index + 1) * group]
        edge_part = jnp.dot(part_cot, w_edge[:, index * group:(index + 1) * group].T, preferred_element_type=jnp.float32)
        edge_part = lax.optimization_barrier(edge_part.astype(jnp.bfloat16))
        edge_total = edge_total + edge_part.astype(jnp.float32)
        grid_part = jnp.dot(part_cot, w_grid[:, index * group:(index + 1) * group].T, preferred_element_type=jnp.float32)
        grid_part = jax.ops.segment_sum(grid_part, senders, num_segments=GRID)
        grid_part = lax.optimization_barrier(grid_part.astype(jnp.bfloat16))
        grid_total = grid_total + grid_part.astype(jnp.float32)
    mesh_terms = jnp.dot(pre_cot, w_mesh.T, preferred_element_type=jnp.float32)
    grad_mesh = jax.ops.segment_sum(mesh_terms, receivers, num_segments=MESH).astype(jnp.bfloat16)
    return (grid_total.astype(jnp.bfloat16), edge_total.astype(jnp.bfloat16), grad_mesh,
            grad_w_grid, grad_w_mesh, grad_w_edge, grad_bias, grad_w_out)
```

```python
import functools

import jax
import jax.numpy as jnp
from jax import lax
from jax.experimental import pallas as pl
from jax.experimental.pallas import tpu as pltpu
from jax.sharding import PartitionSpec as P

BF = jnp.bfloat16
F32 = jnp.float32
MESH = pl.DeviceIdType.MESH
VMEM = pl.BlockSpec(memory_space=pltpu.VMEM)
ANY = pl.BlockSpec(memory_space=pl.ANY)
NN = (((1,), (0,)), ((), ()))
NT = (((1,), (1,)), ((), ()))
TN = (((0,), (0,)), ((), ()))


def mm(a, b, dims=NN):
    return lax.dot_general(a, b, dims, preferred_element_type=F32)


def remote(src, dst, send, recv, device):
    return pltpu.make_async_remote_copy(
        src_ref=src, dst_ref=dst, send_sem=send, recv_sem=recv,
        device_id=device, device_id_type=MESH,
    )


def gather_kernel(
    n, grid, edge, mesh, cot, w_mesh, w_out,
    grid_oth, edge_oth, mesh_oth, cot_oth, win, send, recv,
):
    me, half = lax.axis_index("band"), lax.axis_index("chan")
    up, down = lax.rem(me + 1, n), lax.rem(me + n - 1, n)
    partner = {"band": me, "chan": 1 - half}
    above, below = {"band": up, "chan": half}, {"band": down, "chan": half}
    barrier = pltpu.get_barrier_semaphore()
    for device in (partner, above, below):
        pl.semaphore_signal(barrier, inc=1, device_id=device, device_id_type=MESH)
    pl.semaphore_wait(barrier, 3)
    to_partner = [
        remote(src, dst, send.at[i], recv.at[i], partner)
        for i, (src, dst) in enumerate(
            ((mesh, mesh_oth), (cot, cot_oth), (grid, grid_oth), (edge, edge_oth))
        )
    ]
    for copy in to_partner:
        copy.start()
    rows, hidden = mesh.shape[0], w_mesh.shape[1]
    win[1, :rows, :hidden] = mm(mesh[...], w_mesh[...]).astype(BF)
    win[1, :rows, hidden:] = mm(cot[...], w_out[...], NT).astype(BF)
    to_partner[0].wait()
    to_partner[1].wait()
    win[1, rows:, :hidden] = mm(mesh_oth[...], w_mesh[...]).astype(BF)
    win[1, rows:, hidden:] = mm(cot_oth[...], w_out[...], NT).astype(BF)
    raise_up = remote(win.at[1], win.at[0], send.at[4], recv.at[4], above)
    lower = remote(win.at[1], win.at[2], send.at[5], recv.at[5], below)
    raise_up.start()
    lower.start()
    to_partner[2].wait()
    to_partner[3].wait()
    raise_up.wait()
    lower.wait()


def main_kernel(
    tiles, grid, grid_oth, edge, edge_oth, win, wg_t, we_t, bias, send, recv, live,
    grad_edge, grad_grid, rx, gwg, gwe, gbias,
    pg, pmc, sg, sr, ge, gb,
):
    t = pl.program_id(0)
    rows = grid.shape[0]
    hidden = wg_t.shape[0]
    window = win.shape[0]

    @pl.when(t == 0)
    def _():
        pg[:, :rows] = mm(wg_t[...], grid[...], NT).astype(BF)
        pg[:, rows:2 * rows] = mm(wg_t[...], grid_oth[...], NT).astype(BF)
        pad = pmc.shape[1] - window
        filled = win[...].astype(F32)
        if pad:
            filled = jnp.concatenate([filled, jnp.zeros((pad, 2 * hidden), F32)], axis=0)
        pmc[...] = filled.T.astype(BF)
        sg[...] = jnp.zeros_like(sg)
        sr[...] = jnp.zeros_like(sr)
        ge[...] = jnp.zeros_like(ge)
        gb[...] = jnp.zeros_like(gb)

    tile = edge.shape[0]
    x = jnp.where(t < tiles // 2, edge[...], edge_oth[...])
    s_t = jnp.where(
        lax.broadcasted_iota(jnp.int32, (2 * rows, tile), 0) == send[0], 1.0, 0.0
    ).astype(BF)
    r_t = jnp.where(
        lax.broadcasted_iota(jnp.int32, (pmc.shape[1], tile), 0) == recv[0], 1.0, 0.0
    ).astype(BF)
    both = mm(pmc[...], r_t)
    alive = live[0]
    pre = mm(pg[...], s_t) + both[:hidden] + mm(we_t[...], x, NT) + bias[...]
    sig = jax.nn.sigmoid(pre)
    act = (pre * sig * alive).astype(BF)
    pre_cot32 = both[hidden:] * alive * sig * (1.0 + pre * (1.0 - sig))
    pre_cot = pre_cot32.astype(BF)
    grad_edge[...] = mm(pre_cot, we_t[...], TN).astype(BF)
    sg[...] += mm(pre_cot, s_t, NT)
    sr[...] += mm(jnp.concatenate([pre_cot, act], axis=0), r_t, NT)
    ge[...] += mm(pre_cot, x)
    rounded = pre_cot.astype(F32)
    total = gb[...]
    for k in range(tile // 128):
        total = total + rounded[:, k * 128:(k + 1) * 128]
    gb[...] = total

    @pl.when(t == tiles - 1)
    def _():
        sums = sg[...].astype(BF)
        grad_grid[...] = mm(sums, wg_t[...], TN).astype(BF)
        gwg[...] = (
            mm(sums[:, :rows], grid[...]) + mm(sums[:, rows:], grid_oth[...])
        ).reshape(gwg.shape).astype(BF)
        gwe[...] = ge[...].reshape(gwe.shape).astype(BF)
        rx[...] = sr[...].T[:window].astype(BF)
        gbias[...] = jnp.broadcast_to(
            jnp.sum(gb[...].T, axis=0, keepdims=True), gbias.shape
        )


def reduce_kernel(
    n, grad_edge, grad_grid, rx, gwg, gwe, gbias, mesh, mesh_oth, cot, cot_oth, wm_t,
    edge_in, grid_in, mesh_in, mesh_own, out_a, out_b, bias_all,
    rims, mesh_send, own_b, in_a, in_b, chunk_a, chunk_b,
    send, recv, a_send, a_recv, b_send, b_recv, c_send, c_recv,
):
    me, half = lax.axis_index("band"), lax.axis_index("chan")
    up, down = lax.rem(me + 1, n), lax.rem(me + n - 1, n)
    partner = {"band": me, "chan": 1 - half}
    above, below = {"band": up, "chan": half}, {"band": down, "chan": half}

    def peer(k):
        return lax.rem(me + k, n)

    def device(k):
        return {"band": peer(k), "chan": half}

    def each(fn):
        def step(k, carry):
            fn(k)
            return carry
        lax.fori_loop(1, n, step, 0)

    barrier = pltpu.get_barrier_semaphore()
    pl.semaphore_signal(barrier, inc=1, device_id=partner, device_id_type=MESH)
    each(lambda k: pl.semaphore_signal(
        barrier, inc=1, device_id=device(k), device_id_type=MESH))
    pl.semaphore_wait(barrier, n)

    raise_up = remote(rx.at[2], rims.at[0], send.at[0], recv.at[0], above)
    lower = remote(rx.at[0], rims.at[1], send.at[1], recv.at[1], below)
    raise_up.start()
    lower.start()
    rows_e, rows_g = edge_in.shape[0], grid_in.shape[0]
    edge_copy = remote(
        grad_edge.at[pl.ds(rows_e, rows_e)], edge_in, send.at[2], recv.at[2], partner)
    grid_copy = remote(
        grad_grid.at[pl.ds(rows_g, rows_g)], grid_in, send.at[3], recv.at[3], partner)
    grid_copy.start()
    edge_copy.start()

    def a_copy(k, which, src):
        return remote(src.at[peer(k)], in_a.at[which, k], a_send.at[which, k],
                      a_recv.at[which, k], device(k))

    def bias_copy(k):
        return remote(gbias, bias_all.at[k], a_send.at[2, k], a_recv.at[2, k], device(k))

    def start_a(k):
        a_copy(k, 0, gwg).start()
        a_copy(k, 1, gwe).start()
        bias_copy(k).start()
    each(start_a)
    bias_all[0] = gbias[...]

    raise_up.wait()
    lower.wait()
    total = (rx[1].astype(F32) + rims[0].astype(F32) + rims[1].astype(F32)).astype(BF)
    hidden, rows = wm_t.shape[0], mesh.shape[0]
    mesh_part, act_part = total[:, :hidden], total[:, hidden:]
    part = mm(mesh_part, wm_t[...])
    mesh_send[...] = part[rows:].astype(BF)
    mesh_copy = remote(mesh_send, mesh_in, send.at[4], recv.at[4], partner)
    mesh_copy.start()
    mesh_own[...] = part[:rows].astype(BF)
    own_b[0] = (
        mm(mesh_part[:rows], mesh[...], TN) + mm(mesh_part[rows:], mesh_oth[...], TN)
    ).reshape(own_b.shape[1:]).astype(BF)
    own_b[1] = (
        mm(act_part[:rows], cot[...], TN) + mm(act_part[rows:], cot_oth[...], TN)
    ).reshape(own_b.shape[1:]).astype(BF)

    def b_copy(k, which):
        return remote(own_b.at[which, peer(k)], in_b.at[which, k], b_send.at[which, k],
                      b_recv.at[which, k], device(k))

    def start_b(k):
        b_copy(k, 0).start()
        b_copy(k, 1).start()
    each(start_b)

    def wait_a(k):
        a_copy(k, 0, gwg).wait()
        a_copy(k, 1, gwe).wait()
        bias_copy(k).wait()
    each(wait_a)
    in_a[0, 0] = gwg[me]
    in_a[1, 0] = gwe[me]
    chunk_a[...] = jnp.sum(in_a[...].astype(F32), axis=1).astype(BF)

    def gather_copy(k, which, chunk, out):
        return remote(chunk, out.at[me], c_send.at[which, k], c_recv.at[which, k], device(k))
    each(lambda k: gather_copy(k, 0, chunk_a, out_a).start())
    out_a[me] = chunk_a[...]

    def wait_b(k):
        b_copy(k, 0).wait()
        b_copy(k, 1).wait()
    each(wait_b)
    in_b[0, 0] = own_b[0, me]
    in_b[1, 0] = own_b[1, me]
    chunk_b[...] = jnp.sum(in_b[...].astype(F32), axis=1).astype(BF)
    each(lambda k: gather_copy(k, 1, chunk_b, out_b).start())
    out_b[me] = chunk_b[...]

    grid_copy.wait()
    edge_copy.wait()
    mesh_copy.wait()

    def finish(k):
        gather_copy(k, 0, chunk_a, out_a).wait()
        gather_copy(k, 1, chunk_b, out_b).wait()
    each(finish)


def body(
    grid_latent,
    edge_latent,
    mesh_latent,
    mesh_cotangent,
    w_grid,
    w_mesh,
    w_edge,
    bias,
    w_out,
    senders,
    receivers,
    edge_count,
):
    n = lax.axis_size("band")
    band, chan = lax.axis_index("band"), lax.axis_index("chan")
    rows_g, width = grid_latent.shape
    rows_e = edge_latent.shape[0]
    rows_m = mesh_latent.shape[0]
    hidden = w_grid.shape[1]
    own_m = 2 * rows_m
    sds = jax.ShapeDtypeStruct
    grid_oth, edge_oth, mesh_oth, cot_oth, win = pl.pallas_call(
        functools.partial(gather_kernel, n),
        out_shape=(
            sds(grid_latent.shape, BF), sds(edge_latent.shape, BF),
            sds(mesh_latent.shape, BF), sds(mesh_latent.shape, BF),
            sds((3, own_m, 2 * hidden), BF),
        ),
        in_specs=[ANY, ANY, VMEM, VMEM, VMEM, VMEM],
        out_specs=(ANY, ANY, VMEM, VMEM, VMEM),
        scratch_shapes=[pltpu.SemaphoreType.DMA((6,)), pltpu.SemaphoreType.DMA((6,))],
        compiler_params=pltpu.CompilerParams(collective_id=0, has_side_effects=True),
    )(grid_latent, edge_latent, mesh_latent, mesh_cotangent, w_mesh, w_out)

    tile = 384 if rows_e % 384 == 0 else rows_e
    tiles = 2 * rows_e // tile
    slot = jnp.arange(2 * rows_e, dtype=jnp.int32)
    own_first = lambda v: jnp.roll(v.reshape(2, rows_e), chan, axis=0).reshape(tiles, 1, tile)
    local_send = senders - (band * 2 + chan) * rows_g
    local_send = jnp.where(local_send < 0, local_send + 2 * rows_g, local_send)
    local_recv = receivers - (band - 1) * own_m
    owner, inner = local_recv // own_m, local_recv % own_m
    inner = inner - chan * rows_m
    local_recv = owner * own_m + jnp.where(inner < 0, inner + own_m, inner)
    live = (slot < edge_count[0]).astype(F32)
    pick = lambda v: own_first(v)
    wg_t, we_t, wm_t = w_grid.T, w_edge.T, w_mesh.T
    padded = -(-3 * own_m // 128) * 128
    chunk = hidden * width // (n * 256)
    whole = lambda shape: pl.BlockSpec(shape, lambda t: (0,) * len(shape))
    idx = pl.BlockSpec((1, 1, tile), lambda t: (t, 0, 0))
    mid = tiles // 2
    grad_edge, grad_grid, rx, gwg, gwe, gbias = pl.pallas_call(
        functools.partial(main_kernel, tiles),
        grid=(tiles,),
        out_shape=(
            sds((2 * rows_e, width), BF), sds((2 * rows_g, width), BF),
            sds((3 * own_m, 2 * hidden), BF),
            sds((hidden, width), BF), sds((hidden, width), BF),
            sds((8, hidden), F32),
        ),
        in_specs=[
            whole((rows_g, width)), whole((rows_g, width)),
            pl.BlockSpec((tile, width), lambda t: (jnp.minimum(t, mid - 1), 0)),
            pl.BlockSpec((tile, width), lambda t: (jnp.maximum(t - mid, 0), 0)),
            whole((3 * own_m, 2 * hidden)), whole((hidden, width)), whole((hidden, width)),
            whole((hidden, 1)), idx, idx, idx,
        ],
        out_specs=(
            pl.BlockSpec((tile, width), lambda t: (t, 0)),
            whole((2 * rows_g, width)), whole((3 * own_m, 2 * hidden)),
            whole((hidden, width)), whole((hidden, width)), whole((8, hidden)),
        ),
        scratch_shapes=[
            pltpu.VMEM((hidden, 2 * rows_g), BF), pltpu.VMEM((2 * hidden, padded), BF),
            pltpu.VMEM((hidden, 2 * rows_g), F32), pltpu.VMEM((2 * hidden, padded), F32),
            pltpu.VMEM((hidden, width), F32), pltpu.VMEM((hidden, 128), F32),
        ],
        compiler_params=pltpu.CompilerParams(dimension_semantics=("arbitrary",)),
    )(
        grid_latent, grid_oth, edge_latent, edge_oth,
        win.reshape(3 * own_m, 2 * hidden), wg_t, we_t, bias[:, None],
        pick(local_send), pick(local_recv), pick(live),
    )

    rows_c = hidden // n
    dma = pltpu.SemaphoreType.DMA
    chunked = (n, rows_c, width)
    edge_in, grid_in, mesh_in, mesh_own, out_a, out_b, bias_all = pl.pallas_call(
        functools.partial(reduce_kernel, n),
        out_shape=(
            sds((rows_e, width), BF), sds((rows_g, width), BF),
            sds((rows_m, width), BF), sds((rows_m, width), BF),
            sds((n, 2, rows_c, width), BF), sds((n, 2, rows_c, width), BF),
            sds((n, 8, hidden), F32),
        ),
        in_specs=[ANY, ANY] + [VMEM] * 9,
        out_specs=(ANY, ANY) + (VMEM,) * 5,
        scratch_shapes=[
            pltpu.VMEM((2, own_m, 2 * hidden), BF), pltpu.VMEM((rows_m, width), BF),
            pltpu.VMEM((2,) + chunked, BF), pltpu.VMEM((2,) + chunked, BF),
            pltpu.VMEM((2,) + chunked, BF), pltpu.VMEM((2, rows_c, width), BF),
            pltpu.VMEM((2, rows_c, width), BF),
            dma((5,)), dma((5,)), dma((3, n)), dma((3, n)), dma((2, n)), dma((2, n)),
            dma((2, n)), dma((2, n)),
        ],
        compiler_params=pltpu.CompilerParams(collective_id=1, has_side_effects=True),
    )(
        grad_edge, grad_grid, rx.reshape(3, own_m, 2 * hidden),
        gwg.reshape(chunked), gwe.reshape(chunked), gbias,
        mesh_latent, mesh_oth, mesh_cotangent, cot_oth, wm_t,
    )
    add = lambda a, b: (a.astype(F32) + b.astype(F32)).astype(BF)
    full = lambda out, i: out[:, i].reshape(hidden, width).astype(F32)
    return (
        add(grad_grid[:rows_g], grid_in),
        add(grad_edge[:rows_e], edge_in),
        add(mesh_own, mesh_in),
        full(out_a, 0).T,
        full(out_b, 0).T,
        full(out_a, 1).T,
        jnp.sum(bias_all[:, 0], axis=0),
        full(out_b, 1),
    )


def solution(mesh):
    rows = P(("band", "chan"), None)
    return jax.shard_map(
        body,
        mesh=mesh,
        in_specs=(
            rows, rows, rows, rows,
            P(None, "chan"), P(None, "chan"), P(None, "chan"), P("chan"), P("chan", None),
            P("band"), P("band"), P("band"),
        ),
        out_specs=(
            rows, rows, rows,
            P(None, "chan"), P(None, "chan"), P(None, "chan"), P("chan"), P("chan", None),
        ),
        check_vma=False,
    )
```

```python
import functools

import jax
import jax.numpy as jnp
from jax import lax
from jax.experimental import pallas as pl
from jax.experimental.pallas import tpu as pltpu
from jax.sharding import PartitionSpec as P

BF = jnp.bfloat16
F32 = jnp.float32
MESH = pl.DeviceIdType.MESH
VMEM = pl.BlockSpec(memory_space=pltpu.VMEM)
ANY = pl.BlockSpec(memory_space=pl.ANY)
NN = (((1,), (0,)), ((), ()))
NT = (((1,), (1,)), ((), ()))
TN = (((0,), (0,)), ((), ()))


def mm(a, b, dims=NN):
    return lax.dot_general(a, b, dims, preferred_element_type=F32)


def remote(src, dst, send, recv, device):
    return pltpu.make_async_remote_copy(
        src_ref=src, dst_ref=dst, send_sem=send, recv_sem=recv,
        device_id=device, device_id_type=MESH,
    )


def gather_kernel(n, grid, edge, mesh, cot, grid_oth, edge_oth, win, send, recv, local):
    me, half = lax.axis_index("band"), lax.axis_index("chan")
    up, down = lax.rem(me + 1, n), lax.rem(me + n - 1, n)
    partner = {"band": me, "chan": 1 - half}
    above, below = {"band": up, "chan": half}, {"band": down, "chan": half}
    barrier = pltpu.get_barrier_semaphore()
    for device in (partner, above, below):
        pl.semaphore_signal(barrier, inc=1, device_id=device, device_id_type=MESH)
    pl.semaphore_wait(barrier, 3)
    copies = [
        remote(src, dst, send.at[i], recv.at[i], device)
        for i, (src, dst, device) in enumerate((
            (mesh, win.at[0, 0, 0], above), (cot, win.at[0, 0, 1], above),
            (mesh, win.at[2, 0, 0], below), (cot, win.at[2, 0, 1], below),
            (mesh, win.at[1, 1, 0], partner), (cot, win.at[1, 1, 1], partner),
            (grid, grid_oth, partner), (edge, edge_oth, partner),
        ))
    ]
    own = [
        pltpu.make_async_copy(src, win.at[1, 0, i], local.at[i])
        for i, src in enumerate((mesh, cot))
    ]
    for copy in copies + own:
        copy.start()
    forward = []
    for side in (0, 2):
        copies[side].wait()
        copies[side + 1].wait()
        i = 8 + side // 2
        forward.append(remote(
            win.at[side, 0], win.at[side, 1], send.at[i], recv.at[i], partner))
        forward[-1].start()
    for copy in own + copies[4:] + forward:
        copy.wait()


def turned(x):
    return x.astype(F32).T.astype(BF)


def main_kernel(
    tiles, own_m, scal, grid, grid_oth, edge, edge_oth, win, wg, we, wm, wo, bias, idx,
    grad_edge, grad_grid, rx, gall, gbias,
    wg_t, we_t, bcol, pg, pmc, sg, sr, ge, gb,
):
    t = pl.program_id(0)
    chan, band, count = scal[0], scal[1], scal[2]
    rows, width = grid.shape
    hidden = wg.shape[1]
    window = 3 * own_m
    pad = pmc.shape[1] - window

    def nodes(which):
        rows_in = win[:, :, which].reshape(window, width)
        if pad:
            rows_in = jnp.concatenate([rows_in, jnp.zeros((pad, width), BF)], axis=0)
        return rows_in

    @pl.when(t == 0)
    def _():
        wg_t[...] = turned(wg[...])
        we_t[...] = turned(we[...])
        bcol[...] = jnp.broadcast_to(bias[...], (128, hidden)).T
        pg[:, :rows] = mm(wg_t[...], grid[...], NT).astype(BF)
        pg[:, rows:2 * rows] = mm(wg_t[...], grid_oth[...], NT).astype(BF)
        pmc[:hidden] = mm(nodes(0), wm[...]).T.astype(BF)
        pmc[hidden:] = mm(wo[...], nodes(1), NT).astype(BF)
        sg[...] = jnp.zeros_like(sg)
        sr[...] = jnp.zeros_like(sr)
        ge[...] = jnp.zeros_like(ge)
        gb[...] = jnp.zeros_like(gb)

    tile = edge.shape[0]
    x = jnp.where(t < tiles // 2, edge[...], edge_oth[...])
    place = lax.rem(t + chan * (tiles // 2), tiles)
    from_row = idx[0, 0] - (2 * band + chan) * rows
    from_row = jnp.where(from_row < 0, from_row + 2 * rows, from_row)
    to_row = idx[1, 0] - (band - 1) * own_m
    owner = jnp.where(to_row >= 2 * own_m, 2 * own_m, jnp.where(to_row >= own_m, own_m, 0))
    inner = to_row - owner - chan * (own_m // 2)
    to_row = owner + jnp.where(inner < 0, inner + own_m, inner)
    slot = lax.broadcasted_iota(jnp.int32, (1, tile), 1) + place * tile
    alive = jnp.where(slot < count, 1.0, 0.0)
    s_t = jnp.where(
        lax.broadcasted_iota(jnp.int32, (2 * rows, tile), 0) == from_row, 1.0, 0.0
    ).astype(BF)
    r_t = jnp.where(
        lax.broadcasted_iota(jnp.int32, (pmc.shape[1], tile), 0) == to_row, 1.0, 0.0
    ).astype(BF)
    both = mm(pmc[...], r_t)
    pre = mm(pg[...], s_t) + both[:hidden] + mm(we_t[...], x, NT) + bcol[:, :1]
    sig = jax.nn.sigmoid(pre)
    act = (pre * sig * alive).astype(BF)
    pre_cot = (both[hidden:] * alive * sig * (1.0 + pre * (1.0 - sig))).astype(BF)
    grad_edge[...] = mm(pre_cot, we_t[...], TN).astype(BF)
    sg[...] += mm(pre_cot, s_t, NT)
    sr[...] += mm(jnp.concatenate([pre_cot, act], axis=0), r_t, NT)
    ge[...] += mm(pre_cot, x)
    rounded = pre_cot.astype(F32)
    total = gb[...]
    for k in range(tile // 128):
        total = total + rounded[:, k * 128:(k + 1) * 128]
    gb[...] = total

    @pl.when(t == tiles - 1)
    def _():
        sums = sg[...].astype(BF)
        grad_grid[...] = mm(sums, wg_t[...], TN).astype(BF)
        parts = gall.shape[1:2] + gall.shape[3:]
        put = lambda v: v.reshape(parts).astype(BF)
        gall[0, :, 0] = put(mm(sums[:, :rows], grid[...]) + mm(sums[:, rows:], grid_oth[...]))
        gall[0, :, 1] = put(ge[...])
        mesh_sums = sr[:hidden]
        gall[1, :, 0] = put(mm(mesh_sums.astype(BF), nodes(0)))
        gall[1, :, 1] = put(mm(sr[hidden:].astype(BF), nodes(1)))
        rx[...] = mesh_sums.T[:window].astype(BF)
        gbias[...] = jnp.broadcast_to(
            jnp.sum(gb[...].T, axis=0, keepdims=True), gbias.shape
        )


def reduce_kernel(
    low, high, grad_edge, grad_grid, rx, gall, gbias, wm,
    edge_in, grid_in, mesh_in, mesh_own, out, bias_out,
    rims, mesh_send, in1, sum1, in2, sum2, out1, bias_in, bias_sum,
    send, recv, s1, r1, s2, r2, s3, r3, s4, r4, sb, rb, sc, rc,
):
    n = low * high
    me, half = lax.axis_index("band"), lax.axis_index("chan")
    mine, plane = lax.rem(me, low), me // low
    up, down = lax.rem(me + 1, n), lax.rem(me + n - 1, n)
    partner = {"band": me, "chan": 1 - half}
    above, below = {"band": up, "chan": half}, {"band": down, "chan": half}

    def low_peer(k):
        return lax.rem(mine + k, low)

    def low_device(k):
        return {"band": plane * low + low_peer(k), "chan": half}

    def high_peer(k):
        return lax.rem(plane + k, high)

    def high_device(k):
        return {"band": high_peer(k) * low + mine, "chan": half}

    barrier = pltpu.get_barrier_semaphore()

    def greet(k, carry):
        pl.semaphore_signal(
            barrier, inc=1, device_id={"band": lax.rem(me + k, n), "chan": half},
            device_id_type=MESH)
        return carry
    pl.semaphore_signal(barrier, inc=1, device_id=partner, device_id_type=MESH)
    lax.fori_loop(1, n, greet, 0)
    pl.semaphore_wait(barrier, n)

    def scatter_low(k, ab):
        return remote(gall.at[ab, low_peer(k)], in1.at[ab, k], s1.at[ab, k], r1.at[ab, k],
                      low_device(k))

    def scatter_high(k, ab):
        return remote(sum1.at[ab, high_peer(k)], in2.at[ab, k], s2.at[ab, k], r2.at[ab, k],
                      high_device(k))

    def gather_high(k, ab):
        return remote(sum2.at[ab], out1.at[ab, plane], s3.at[ab, k], r3.at[ab, k],
                      high_device(k))

    def gather_low(k, ab):
        return remote(out1.at[ab], out.at[ab, mine], s4.at[ab, k], r4.at[ab, k],
                      low_device(k))

    def bias_low(k):
        return remote(gbias, bias_in.at[mine], sb.at[k], rb.at[k], low_device(k))

    def bias_high(k):
        return remote(bias_sum, bias_out.at[plane], sc.at[k], rc.at[k], high_device(k))

    lows, highs = range(1, low), range(1, high)
    for k in lows:
        scatter_low(k, 0).start()
    for k in lows:
        bias_low(k).start()
    raise_up = remote(rx.at[2], rims.at[0], send.at[0], recv.at[0], above)
    lower = remote(rx.at[0], rims.at[1], send.at[1], recv.at[1], below)
    rows_e, rows_g, rows_m = edge_in.shape[0], grid_in.shape[0], mesh_own.shape[0]
    edge_copy = remote(
        grad_edge.at[pl.ds(rows_e, rows_e)], edge_in, send.at[2], recv.at[2], partner)
    grid_copy = remote(
        grad_grid.at[pl.ds(rows_g, rows_g)], grid_in, send.at[3], recv.at[3], partner)
    for k in lows:
        scatter_low(k, 1).start()
    grid_copy.start()
    edge_copy.start()
    raise_up.start()
    lower.start()
    bias_in[mine] = gbias[...]

    def reduce_low(ab):
        for k in lows:
            scatter_low(k, ab).wait()
        total = gall[ab, mine].astype(F32)
        for k in lows:
            total = total + in1[ab, k].astype(F32)
        sum1[ab] = total.astype(BF)
        for k in highs:
            scatter_high(k, ab).start()

    def reduce_high(ab):
        for k in highs:
            scatter_high(k, ab).wait()
        total = sum1[ab, plane].astype(F32)
        for k in highs:
            total = total + in2[ab, k].astype(F32)
        sum2[ab] = total.astype(BF)
        for k in highs:
            gather_high(k, ab).start()
        out1[ab, plane] = sum2[ab]

    def spread(ab):
        for k in highs:
            gather_high(k, ab).wait()
        for k in lows:
            gather_low(k, ab).start()
        out[ab, mine] = out1[ab]

    reduce_low(0)
    for k in lows:
        bias_low(k).wait()
    bias_sum[...] = jnp.sum(bias_in[...], axis=0)
    for k in highs:
        bias_high(k).start()
    bias_out[plane] = bias_sum[...]
    reduce_high(0)
    reduce_low(1)
    spread(0)
    reduce_high(1)
    raise_up.wait()
    lower.wait()
    total = (rx[1].astype(F32) + rims[0].astype(F32) + rims[1].astype(F32)).astype(BF)
    part = mm(total, wm[...], NT)
    mesh_send[...] = part[rows_m:].astype(BF)
    mesh_copy = remote(mesh_send, mesh_in, send.at[4], recv.at[4], partner)
    mesh_copy.start()
    mesh_own[...] = part[:rows_m].astype(BF)
    spread(1)
    grid_copy.wait()
    edge_copy.wait()
    mesh_copy.wait()
    for k in highs:
        bias_high(k).wait()
    for ab in (0, 1):
        for k in lows:
            gather_low(k, ab).wait()


def final_kernel(
    grid_own, grid_in, edge_own, edge_in, mesh_own, mesh_in, out, bias_out,
    grad_grid, grad_edge, grad_mesh, gwg, gwm, gwe, gbias, gwo,
):
    for a, b, to in (
        (grid_own, grid_in, grad_grid), (edge_own, edge_in, grad_edge),
        (mesh_own, mesh_in, grad_mesh),
    ):
        to[...] = (a[...].astype(F32) + b[...].astype(F32)).astype(BF)
    full = lambda ab, i: out[ab, :, i].astype(F32).reshape(gwo.shape)
    gwg[...] = full(0, 0).T
    gwe[...] = full(0, 1).T
    gwm[...] = full(1, 0).T
    gwo[...] = full(1, 1)
    gbias[...] = jnp.sum(bias_out[...], axis=0)


def body(
    grid_latent,
    edge_latent,
    mesh_latent,
    mesh_cotangent,
    w_grid,
    w_mesh,
    w_edge,
    bias,
    w_out,
    senders,
    receivers,
    edge_count,
):
    n = lax.axis_size("band")
    band, chan = lax.axis_index("band"), lax.axis_index("chan")
    rows_g, width = grid_latent.shape
    rows_e = edge_latent.shape[0]
    rows_m = mesh_latent.shape[0]
    hidden = w_grid.shape[1]
    own_m = 2 * rows_m
    sds = jax.ShapeDtypeStruct
    dma = pltpu.SemaphoreType.DMA
    grid_oth, edge_oth, win = pl.pallas_call(
        functools.partial(gather_kernel, n),
        out_shape=(
            sds(grid_latent.shape, BF), sds(edge_latent.shape, BF),
            sds((3, 2, 2, rows_m, width), BF),
        ),
        in_specs=[ANY, ANY, VMEM, VMEM],
        out_specs=(ANY, ANY, VMEM),
        scratch_shapes=[dma((10,)), dma((10,)), dma((2,))],
        compiler_params=pltpu.CompilerParams(collective_id=0, has_side_effects=True),
    )(grid_latent, edge_latent, mesh_latent, mesh_cotangent)

    tile = 384 if rows_e % 384 == 0 else rows_e
    tiles = 2 * rows_e // tile
    mid = tiles // 2
    padded = -(-3 * own_m // 128) * 128
    low = 1
    while low * low < n:
        low *= 2
    high = n // low
    rows_c = hidden // n
    scal = jnp.stack([chan, band, edge_count[0]]).astype(jnp.int32)
    idx = jnp.stack([senders, receivers]).reshape(2, tiles, 1, tile)
    whole = lambda *shape: pl.BlockSpec(shape, lambda t, s: (0,) * len(shape))
    grad_edge, grad_grid, rx, gall, gbias = pl.pallas_call(
        functools.partial(main_kernel, tiles, own_m),
        grid_spec=pltpu.PrefetchScalarGridSpec(
            num_scalar_prefetch=1,
            grid=(tiles,),
            in_specs=[
                whole(rows_g, width), whole(rows_g, width),
                pl.BlockSpec((tile, width), lambda t, s: (jnp.minimum(t, mid - 1), 0)),
                pl.BlockSpec((tile, width), lambda t, s: (jnp.maximum(t - mid, 0), 0)),
                whole(3, 2, 2, rows_m, width),
                whole(width, hidden), whole(width, hidden), whole(width, hidden),
                whole(hidden, width), whole(1, hidden),
                pl.BlockSpec(
                    (2, 1, 1, tile), lambda t, s: (0, lax.rem(t + s[0] * mid, tiles), 0, 0)),
            ],
            out_specs=(
                pl.BlockSpec((tile, width), lambda t, s: (t, 0)),
                whole(2 * rows_g, width), whole(3 * own_m, hidden),
                whole(2, n, 2, rows_c, width), whole(8, hidden),
            ),
            scratch_shapes=[
                pltpu.VMEM((hidden, width), BF), pltpu.VMEM((hidden, width), BF),
                pltpu.VMEM((hidden, 128), F32),
                pltpu.VMEM((hidden, 2 * rows_g), BF), pltpu.VMEM((2 * hidden, padded), BF),
                pltpu.VMEM((hidden, 2 * rows_g), F32), pltpu.VMEM((2 * hidden, padded), F32),
                pltpu.VMEM((hidden, width), F32), pltpu.VMEM((hidden, 128), F32),
            ],
        ),
        out_shape=(
            sds((2 * rows_e, width), BF), sds((2 * rows_g, width), BF),
            sds((3 * own_m, hidden), BF),
            sds((2, n, 2, rows_c, width), BF), sds((8, hidden), F32),
        ),
        compiler_params=pltpu.CompilerParams(dimension_semantics=("arbitrary",)),
    )(
        scal, grid_latent, grid_oth, edge_latent, edge_oth, win,
        w_grid, w_edge, w_mesh, w_out, bias[None], idx,
    )

    blocks = (2, rows_c, width)
    edge_in, grid_in, mesh_in, mesh_own, out, bias_out = pl.pallas_call(
        functools.partial(reduce_kernel, low, high),
        out_shape=(
            sds((rows_e, width), BF), sds((rows_g, width), BF),
            sds((rows_m, width), BF), sds((rows_m, width), BF),
            sds((2, low, high) + blocks, BF), sds((high, 8, hidden), F32),
        ),
        in_specs=[ANY, ANY] + [VMEM] * 4,
        out_specs=(ANY, ANY) + (VMEM,) * 4,
        scratch_shapes=[
            pltpu.VMEM((2, own_m, hidden), BF), pltpu.VMEM((rows_m, width), BF),
            pltpu.VMEM((2, low, high) + blocks, BF), pltpu.VMEM((2, high) + blocks, BF),
            pltpu.VMEM((2, high) + blocks, BF), pltpu.VMEM((2,) + blocks, BF),
            pltpu.VMEM((2, high) + blocks, BF),
            pltpu.VMEM((low, 8, hidden), F32), pltpu.VMEM((8, hidden), F32),
            dma((5,)), dma((5,)), dma((2, low)), dma((2, low)), dma((2, high)),
            dma((2, high)), dma((2, high)), dma((2, high)), dma((2, low)), dma((2, low)),
            dma((low,)), dma((low,)), dma((high,)), dma((high,)),
        ],
        compiler_params=pltpu.CompilerParams(collective_id=1, has_side_effects=True),
    )(
        grad_edge, grad_grid, rx.reshape(3, own_m, hidden),
        gall.reshape((2, low, high) + blocks), gbias, w_mesh,
    )

    rows_of = lambda rows: pl.BlockSpec((rows // 2, width), lambda t: (t, 0))
    turned_spec = pl.BlockSpec((width, hidden // 2), lambda t: (0, t))
    grad_grid, grad_edge, grad_mesh, gwg, gwm, gwe, gbias, gwo = pl.pallas_call(
        final_kernel,
        grid=(2,),
        in_specs=[
            rows_of(rows_g), rows_of(rows_g), rows_of(rows_e), rows_of(rows_e),
            rows_of(rows_m), rows_of(rows_m),
            pl.BlockSpec((2, n // 2) + blocks, lambda t: (0, t, 0, 0, 0)),
            pl.BlockSpec((high, 8, hidden), lambda t: (0, 0, 0)),
        ],
        out_specs=(
            rows_of(rows_g), rows_of(rows_e), rows_of(rows_m),
            turned_spec, turned_spec, turned_spec,
            pl.BlockSpec((8, hidden), lambda t: (0, 0)), rows_of(hidden),
        ),
        out_shape=(
            sds((rows_g, width), BF), sds((rows_e, width), BF), sds((rows_m, width), BF),
            sds((width, hidden), F32), sds((width, hidden), F32), sds((width, hidden), F32),
            sds((8, hidden), F32), sds((hidden, width), F32),
        ),
        compiler_params=pltpu.CompilerParams(dimension_semantics=("arbitrary",)),
    )(
        grad_grid, grid_in, grad_edge, edge_in, mesh_own, mesh_in,
        out.reshape((2, n) + blocks), bias_out,
    )
    return grad_grid, grad_edge, grad_mesh, gwg, gwm, gwe, gbias[0], gwo


def solution(mesh):
    rows = P(("band", "chan"), None)
    return jax.shard_map(
        body,
        mesh=mesh,
        in_specs=(
            rows, rows, rows, rows,
            P(None, "chan"), P(None, "chan"), P(None, "chan"), P("chan"), P("chan", None),
            P("band"), P("band"), P("band"),
        ),
        out_specs=(
            rows, rows, rows,
            P(None, "chan"), P(None, "chan"), P(None, "chan"), P("chan"), P("chan", None),
        ),
        check_vma=False,
    )
```

```python
import functools

import jax
import jax.numpy as jnp
from jax import lax
from jax.experimental import pallas as pl
from jax.experimental.pallas import tpu as pltpu
from jax.sharding import PartitionSpec as P

BF = jnp.bfloat16
F32 = jnp.float32
MESH = pl.DeviceIdType.MESH
VMEM = pl.BlockSpec(memory_space=pltpu.VMEM)
ANY = pl.BlockSpec(memory_space=pl.ANY)
NN = (((1,), (0,)), ((), ()))
NT = (((1,), (1,)), ((), ()))
TN = (((0,), (0,)), ((), ()))


def mm(a, b, dims=NN):
    return lax.dot_general(a, b, dims, preferred_element_type=F32)


def remote(src, dst, send, recv, device):
    return pltpu.make_async_remote_copy(
        src_ref=src, dst_ref=dst, send_sem=send, recv_sem=recv,
        device_id=device, device_id_type=MESH,
    )


def gather_kernel(n, grid, edge, mesh, cot, grid_oth, edge_oth, win, send, recv, local):
    me, half = lax.axis_index("band"), lax.axis_index("chan")
    up, down = lax.rem(me + 1, n), lax.rem(me + n - 1, n)
    partner = {"band": me, "chan": 1 - half}
    above, below = {"band": up, "chan": half}, {"band": down, "chan": half}
    barrier = pltpu.get_barrier_semaphore()
    for device in (partner, above, below):
        pl.semaphore_signal(barrier, inc=1, device_id=device, device_id_type=MESH)
    pl.semaphore_wait(barrier, 3)
    copies = [
        remote(src, dst, send.at[i], recv.at[i], device)
        for i, (src, dst, device) in enumerate((
            (mesh, win.at[0, 0, 0], above), (cot, win.at[0, 0, 1], above),
            (mesh, win.at[2, 0, 0], below), (cot, win.at[2, 0, 1], below),
            (mesh, win.at[1, 1, 0], partner), (cot, win.at[1, 1, 1], partner),
            (grid, grid_oth, partner), (edge, edge_oth, partner),
        ))
    ]
    own = [
        pltpu.make_async_copy(src, win.at[1, 0, i], local.at[i])
        for i, src in enumerate((mesh, cot))
    ]
    for copy in copies + own:
        copy.start()
    forward = []
    for side in (0, 2):
        copies[side].wait()
        copies[side + 1].wait()
        i = 8 + side // 2
        forward.append(remote(
            win.at[side, 0], win.at[side, 1], send.at[i], recv.at[i], partner))
        forward[-1].start()
    for copy in own + copies[4:] + forward:
        copy.wait()


def turned(x):
    return x.astype(F32).T.astype(BF)


def main_kernel(
    tiles, own_m, used, grid, grid_oth, edge, edge_oth, win, wg, we, wm, wo, bias, sender, receiver,
    grad_edge, grad_grid, rx, gall, gbias,
    wg_t, we_t, bcol, pg, pmc, sg, sr, ge, gb,
):
    t = pl.program_id(0)
    chan, band, count = lax.axis_index("chan"), lax.axis_index("band"), used[0]
    rows, width = grid.shape
    hidden = wg.shape[1]
    window = 3 * own_m
    pad = pmc.shape[1] - window

    def nodes(which):
        rows_in = win[:, :, which].reshape(window, width)
        if pad:
            rows_in = jnp.concatenate([rows_in, jnp.zeros((pad, width), BF)], axis=0)
        return rows_in

    @pl.when(t == 0)
    def _():
        wg_t[...] = turned(wg[...])
        we_t[...] = turned(we[...])
        bcol[...] = jnp.broadcast_to(bias[...], (128, hidden)).T
        pg[:, :rows] = mm(wg_t[...], grid[...], NT).astype(BF)
        pg[:, rows:2 * rows] = mm(wg_t[...], grid_oth[...], NT).astype(BF)
        pmc[:hidden] = mm(nodes(0), wm[...]).T.astype(BF)
        pmc[hidden:] = mm(wo[...], nodes(1), NT).astype(BF)
        sg[...] = jnp.zeros_like(sg)
        sr[...] = jnp.zeros_like(sr)
        ge[...] = jnp.zeros_like(ge)
        gb[...] = jnp.zeros_like(gb)

    tile = edge.shape[0]
    x = jnp.where(t < tiles // 2, edge[...], edge_oth[...])
    place = lax.rem(t + chan * (tiles // 2), tiles)
    from_row = sender[place] - (2 * band + chan) * rows
    from_row = jnp.where(from_row < 0, from_row + 2 * rows, from_row)
    to_row = receiver[place] - (band - 1) * own_m
    owner = jnp.where(to_row >= 2 * own_m, 2 * own_m, jnp.where(to_row >= own_m, own_m, 0))
    inner = to_row - owner - chan * (own_m // 2)
    to_row = owner + jnp.where(inner < 0, inner + own_m, inner)
    slot = lax.broadcasted_iota(jnp.int32, (1, tile), 1) + place * tile
    alive = jnp.where(slot < count, 1.0, 0.0)
    s_t = jnp.where(
        lax.broadcasted_iota(jnp.int32, (2 * rows, tile), 0) == from_row, 1.0, 0.0
    ).astype(BF)
    r_t = jnp.where(
        lax.broadcasted_iota(jnp.int32, (pmc.shape[1], tile), 0) == to_row, 1.0, 0.0
    ).astype(BF)
    both = mm(pmc[...], r_t)
    pre = mm(pg[...], s_t) + both[:hidden] + mm(we_t[...], x, NT) + bcol[:, :1]
    sig = jax.nn.sigmoid(pre)
    act = (pre * sig * alive).astype(BF)
    pre_cot = (both[hidden:] * alive * sig * (1.0 + pre * (1.0 - sig))).astype(BF)
    grad_edge[...] = mm(pre_cot, we_t[...], TN).astype(BF)
    sg[...] += mm(pre_cot, s_t, NT)
    sr[...] += mm(jnp.concatenate([pre_cot, act], axis=0), r_t, NT)
    ge[...] += mm(pre_cot, x)
    rounded = pre_cot.astype(F32)
    total = gb[...]
    for k in range(tile // 128):
        total = total + rounded[:, k * 128:(k + 1) * 128]
    gb[...] = total

    @pl.when(t == tiles - 1)
    def _():
        sums = sg[...].astype(BF)
        grad_grid[...] = mm(sums, wg_t[...], TN).astype(BF)
        parts = gall.shape[1:2] + gall.shape[3:]
        put = lambda v: v.reshape(parts).astype(BF)
        gall[0, :, 0] = put(mm(sums[:, :rows], grid[...]) + mm(sums[:, rows:], grid_oth[...]))
        gall[0, :, 1] = put(ge[...])
        mesh_sums = sr[:hidden]
        gall[1, :, 0] = put(mm(mesh_sums.astype(BF), nodes(0)))
        gall[1, :, 1] = put(mm(sr[hidden:].astype(BF), nodes(1)))
        rx[...] = mesh_sums.T[:window].astype(BF)
        gbias[...] = jnp.broadcast_to(
            jnp.sum(gb[...].T, axis=0, keepdims=True), gbias.shape
        )


def reduce_kernel(
    low, high, grad_edge, grad_grid, rx, gall, gbias, wm,
    edge_in, grid_in, mesh_in, mesh_own, out, bias_out,
    rims, mesh_send, in1, sum1, in2, sum2, out1, bias_in, bias_sum,
    send, recv, s1, r1, s2, r2, s3, r3, s4, r4, sb, rb, sc, rc,
):
    n = low * high
    me, half = lax.axis_index("band"), lax.axis_index("chan")
    mine, plane = lax.rem(me, low), me // low
    up, down = lax.rem(me + 1, n), lax.rem(me + n - 1, n)
    partner = {"band": me, "chan": 1 - half}
    above, below = {"band": up, "chan": half}, {"band": down, "chan": half}

    def low_peer(k):
        return lax.rem(mine + k, low)

    def low_device(k):
        return {"band": plane * low + low_peer(k), "chan": half}

    def high_peer(k):
        return lax.rem(plane + k, high)

    def high_device(k):
        return {"band": high_peer(k) * low + mine, "chan": half}

    barrier = pltpu.get_barrier_semaphore()

    def greet(k, carry):
        pl.semaphore_signal(
            barrier, inc=1, device_id={"band": lax.rem(me + k, n), "chan": half},
            device_id_type=MESH)
        return carry
    pl.semaphore_signal(barrier, inc=1, device_id=partner, device_id_type=MESH)
    lax.fori_loop(1, n, greet, 0)
    pl.semaphore_wait(barrier, n)

    def scatter_low(k, ab):
        return remote(gall.at[ab, low_peer(k)], in1.at[ab, k], s1.at[ab, k], r1.at[ab, k],
                      low_device(k))

    def scatter_high(k, ab):
        return remote(sum1.at[ab, high_peer(k)], in2.at[ab, k], s2.at[ab, k], r2.at[ab, k],
                      high_device(k))

    def gather_high(k, ab):
        return remote(sum2.at[ab], out1.at[ab, plane], s3.at[ab, k], r3.at[ab, k],
                      high_device(k))

    def gather_low(k, ab):
        return remote(out1.at[ab], out.at[ab, mine], s4.at[ab, k], r4.at[ab, k],
                      low_device(k))

    def bias_low(k):
        return remote(gbias, bias_in.at[mine], sb.at[k], rb.at[k], low_device(k))

    def bias_high(k):
        return remote(bias_sum, bias_out.at[plane], sc.at[k], rc.at[k], high_device(k))

    lows, highs = range(1, low), range(1, high)
    for k in lows:
        scatter_low(k, 0).start()
    for k in lows:
        bias_low(k).start()
    raise_up = remote(rx.at[2], rims.at[0], send.at[0], recv.at[0], above)
    lower = remote(rx.at[0], rims.at[1], send.at[1], recv.at[1], below)
    rows_e, rows_g, rows_m = edge_in.shape[0], grid_in.shape[0], mesh_own.shape[0]
    edge_copy = remote(
        grad_edge.at[pl.ds(rows_e, rows_e)], edge_in, send.at[2], recv.at[2], partner)
    grid_copy = remote(
        grad_grid.at[pl.ds(rows_g, rows_g)], grid_in, send.at[3], recv.at[3], partner)
    for k in lows:
        scatter_low(k, 1).start()
    grid_copy.start()
    edge_copy.start()
    raise_up.start()
    lower.start()
    bias_in[mine] = gbias[...]

    def reduce_low(ab):
        for k in lows:
            scatter_low(k, ab).wait()
        total = gall[ab, mine].astype(F32)
        for k in lows:
            total = total + in1[ab, k].astype(F32)
        sum1[ab] = total.astype(BF)
        for k in highs:
            scatter_high(k, ab).start()

    def reduce_high(ab):
        for k in highs:
            scatter_high(k, ab).wait()
        total = sum1[ab, plane].astype(F32)
        for k in highs:
            total = total + in2[ab, k].astype(F32)
        sum2[ab] = total.astype(BF)
        for k in highs:
            gather_high(k, ab).start()
        out1[ab, plane] = sum2[ab]

    def spread(ab):
        for k in highs:
            gather_high(k, ab).wait()
        for k in lows:
            gather_low(k, ab).start()
        out[ab, mine] = out1[ab]

    reduce_low(0)
    for k in lows:
        bias_low(k).wait()
    bias_sum[...] = jnp.sum(bias_in[...], axis=0)
    for k in highs:
        bias_high(k).start()
    bias_out[plane] = bias_sum[...]
    reduce_high(0)
    reduce_low(1)
    spread(0)
    reduce_high(1)
    raise_up.wait()
    lower.wait()
    total = (rx[1].astype(F32) + rims[0].astype(F32) + rims[1].astype(F32)).astype(BF)
    part = mm(total, wm[...], NT)
    mesh_send[...] = part[rows_m:].astype(BF)
    mesh_copy = remote(mesh_send, mesh_in, send.at[4], recv.at[4], partner)
    mesh_copy.start()
    mesh_own[...] = part[:rows_m].astype(BF)
    spread(1)
    grid_copy.wait()
    edge_copy.wait()
    mesh_copy.wait()
    for k in highs:
        bias_high(k).wait()
    for ab in (0, 1):
        for k in lows:
            gather_low(k, ab).wait()


def final_kernel(
    grid_own, grid_in, edge_own, edge_in, mesh_own, mesh_in, out, bias_out,
    grad_grid, grad_edge, grad_mesh, gwg, gwm, gwe, gbias, gwo,
):
    for a, b, to in (
        (grid_own, grid_in, grad_grid), (edge_own, edge_in, grad_edge),
        (mesh_own, mesh_in, grad_mesh),
    ):
        to[...] = (a[...].astype(F32) + b[...].astype(F32)).astype(BF)
    full = lambda ab, i: out[ab, :, i].astype(F32).reshape(gwo.shape)
    gwg[...] = full(0, 0).T
    gwe[...] = full(0, 1).T
    gwm[...] = full(1, 0).T
    gwo[...] = full(1, 1)
    gbias[...] = jnp.sum(bias_out[...], axis=0)[0]


def body(
    grid_latent,
    edge_latent,
    mesh_latent,
    mesh_cotangent,
    w_grid,
    w_mesh,
    w_edge,
    bias,
    w_out,
    senders,
    receivers,
    edge_count,
):
    n = lax.axis_size("band")
    rows_g, width = grid_latent.shape
    rows_e = edge_latent.shape[0]
    rows_m = mesh_latent.shape[0]
    hidden = w_grid.shape[1]
    own_m = 2 * rows_m
    sds = jax.ShapeDtypeStruct
    dma = pltpu.SemaphoreType.DMA
    grid_oth, edge_oth, win = pl.pallas_call(
        functools.partial(gather_kernel, n),
        out_shape=(
            sds(grid_latent.shape, BF), sds(edge_latent.shape, BF),
            sds((3, 2, 2, rows_m, width), BF),
        ),
        in_specs=[ANY, ANY, VMEM, VMEM],
        out_specs=(ANY, ANY, VMEM),
        scratch_shapes=[dma((10,)), dma((10,)), dma((2,))],
        compiler_params=pltpu.CompilerParams(collective_id=0, has_side_effects=True),
    )(grid_latent, edge_latent, mesh_latent, mesh_cotangent)

    tile = rows_e
    tiles = 2 * rows_e // tile
    mid = tiles // 2
    padded = -(-3 * own_m // 128) * 128
    low = 1
    while low * low < n:
        low *= 2
    high = n // low
    rows_c = hidden // n
    whole = lambda *shape: pl.BlockSpec(shape, lambda t: (0,) * len(shape))
    grad_edge, grad_grid, rx, gall, gbias = pl.pallas_call(
        functools.partial(main_kernel, tiles, own_m),
        grid=(tiles,),
        in_specs=[
            pl.BlockSpec(memory_space=pltpu.SMEM),
            whole(rows_g, width), whole(rows_g, width),
            pl.BlockSpec((tile, width), lambda t: (jnp.minimum(t, mid - 1), 0)),
            pl.BlockSpec((tile, width), lambda t: (jnp.maximum(t - mid, 0), 0)),
            whole(3, 2, 2, rows_m, width),
            whole(width, hidden), whole(width, hidden), whole(width, hidden),
            whole(hidden, width), whole(1, hidden),
            whole(tiles, 1, tile), whole(tiles, 1, tile),
        ],
        out_specs=(
            pl.BlockSpec((tile, width), lambda t: (t, 0)),
            whole(2 * rows_g, width), whole(3 * own_m, hidden),
            whole(2, n, 2, rows_c, width), whole(8, hidden),
        ),
        scratch_shapes=[
            pltpu.VMEM((hidden, width), BF), pltpu.VMEM((hidden, width), BF),
            pltpu.VMEM((hidden, 128), F32),
            pltpu.VMEM((hidden, 2 * rows_g), BF), pltpu.VMEM((2 * hidden, padded), BF),
            pltpu.VMEM((hidden, 2 * rows_g), F32), pltpu.VMEM((2 * hidden, padded), F32),
            pltpu.VMEM((hidden, width), F32), pltpu.VMEM((hidden, 128), F32),
        ],
        out_shape=(
            sds((2 * rows_e, width), BF), sds((2 * rows_g, width), BF),
            sds((3 * own_m, hidden), BF),
            sds((2, n, 2, rows_c, width), BF), sds((8, hidden), F32),
        ),
        compiler_params=pltpu.CompilerParams(dimension_semantics=("arbitrary",)),
    )(
        edge_count, grid_latent, grid_oth, edge_latent, edge_oth, win,
        w_grid, w_edge, w_mesh, w_out, bias[None],
        senders.reshape(tiles, 1, tile), receivers.reshape(tiles, 1, tile),
    )

    blocks = (2, rows_c, width)
    edge_in, grid_in, mesh_in, mesh_own, out, bias_out = pl.pallas_call(
        functools.partial(reduce_kernel, low, high),
        out_shape=(
            sds((rows_e, width), BF), sds((rows_g, width), BF),
            sds((rows_m, width), BF), sds((rows_m, width), BF),
            sds((2, low, high) + blocks, BF), sds((high, 8, hidden), F32),
        ),
        in_specs=[ANY, ANY] + [VMEM] * 4,
        out_specs=(ANY, ANY) + (VMEM,) * 4,
        scratch_shapes=[
            pltpu.VMEM((2, own_m, hidden), BF), pltpu.VMEM((rows_m, width), BF),
            pltpu.VMEM((2, low, high) + blocks, BF), pltpu.VMEM((2, high) + blocks, BF),
            pltpu.VMEM((2, high) + blocks, BF), pltpu.VMEM((2,) + blocks, BF),
            pltpu.VMEM((2, high) + blocks, BF),
            pltpu.VMEM((low, 8, hidden), F32), pltpu.VMEM((8, hidden), F32),
            dma((5,)), dma((5,)), dma((2, low)), dma((2, low)), dma((2, high)),
            dma((2, high)), dma((2, high)), dma((2, high)), dma((2, low)), dma((2, low)),
            dma((low,)), dma((low,)), dma((high,)), dma((high,)),
        ],
        compiler_params=pltpu.CompilerParams(collective_id=1, has_side_effects=True),
    )(
        grad_edge, grad_grid, rx.reshape(3, own_m, hidden),
        gall.reshape((2, low, high) + blocks), gbias, w_mesh,
    )

    rows_of = lambda rows: pl.BlockSpec((rows // 2, width), lambda t: (t, 0))
    turned_spec = pl.BlockSpec((width, hidden // 2), lambda t: (0, t))
    grad_grid, grad_edge, grad_mesh, gwg, gwm, gwe, gbias, gwo = pl.pallas_call(
        final_kernel,
        grid=(2,),
        in_specs=[
            rows_of(rows_g), rows_of(rows_g), rows_of(rows_e), rows_of(rows_e),
            rows_of(rows_m), rows_of(rows_m),
            pl.BlockSpec((2, n // 2) + blocks, lambda t: (0, t, 0, 0, 0)),
            pl.BlockSpec((high, 8, hidden), lambda t: (0, 0, 0)),
        ],
        out_specs=(
            rows_of(rows_g), rows_of(rows_e), rows_of(rows_m),
            turned_spec, turned_spec, turned_spec,
            pl.BlockSpec((hidden,), lambda t: (0,)), rows_of(hidden),
        ),
        out_shape=(
            sds((rows_g, width), BF), sds((rows_e, width), BF), sds((rows_m, width), BF),
            sds((width, hidden), F32), sds((width, hidden), F32), sds((width, hidden), F32),
            sds((hidden,), F32), sds((hidden, width), F32),
        ),
        compiler_params=pltpu.CompilerParams(dimension_semantics=("arbitrary",)),
    )(
        grad_grid, grid_in, grad_edge, edge_in, mesh_own, mesh_in,
        out.reshape((2, n) + blocks), bias_out,
    )
    return grad_grid, grad_edge, grad_mesh, gwg, gwm, gwe, gbias, gwo


def solution(mesh):
    rows = P(("band", "chan"), None)
    return jax.shard_map(
        body,
        mesh=mesh,
        in_specs=(
            rows, rows, rows, rows,
            P(None, "chan"), P(None, "chan"), P(None, "chan"), P("chan"), P("chan", None),
            P("band"), P("band"), P("band"),
        ),
        out_specs=(
            rows, rows, rows,
            P(None, "chan"), P(None, "chan"), P(None, "chan"), P("chan"), P("chan", None),
        ),
        check_vma=False,
    )
```
